32 devices in a mesh: grp: 2 (over y), sp: 4 (over z), sub: 2 (over x), rep: 2 (over core).
Axes of the slice: x: 2, y: 2, z: 4, core: 2. Of those that a mesh axis runs over, the one named last changes fastest.
Arguments:
- field: float32 [512, 32, 32, 128], P(('grp', 'sp', 'rep'), 'sub'), parts along dimension 0, may hold values from -40 to 40, as said below
- mix_weight: float32 [256, 256], replicated, may hold values from -0.375 to 0.375
- factor_x: float32 [256, 32], replicated, may hold values from -6 to 6
- factor_y: float32 [256, 32], replicated, may hold values from -6 to 6
- factor_z: float32 [256, 32], replicated, may hold values from -6 to 6
- norm_gain: float32 [256], replicated, may hold values from 0.5 to 1.5
- norm_bias: float32 [256], replicated, may hold values from -3 to 3
- w_in: float32 [256, 256], replicated, may hold values from -0.375 to 0.375
- b_in: float32 [256], replicated, may hold values from -3 to 3
- w_out: float32 [256, 256], replicated, may hold values from -0.375 to 0.375
- b_out: float32 [256], replicated, may hold values from -3 to 3
Outputs:
- block_out: float32 [512, 32, 32, 128], P('grp', 'sub', ('sp', 'rep')), parts along dimension 0
The draws below stay inside these ranges and needn't reach their ends.
There are 2 independent parts, one for each index of `grp`. The reference program is written for one: setup_inputs(seed, part) draws one part's arguments, and reference() takes and returns one part's arrays. A program takes and returns all parts, laid end to end along the dimension named above; an argument that names none is the same for every part. Nothing has to cross between parts.
Inputs may be any that keep to these rules, and one draw needn't show every extreme that they name: `field`: real values of order one in each channel, with scales that differ between channels.
All inputs are finite; a program needn't handle non-finite values.
Results may differ from the reference program's by a relative error of at most 0.000078.
Values sent between devices are 32-bit elements; how exact they have to be, the bound alone decides.
A program may use at most 128 MiB of HBM per device.

```python
import math
import jax
import jax.numpy as jnp
from jax import lax

C = 256
HID = 256
KX = 32
KY = 32
KZ = 32
GROUPS = 32
NX = 32
NY = 32
NZ = 128


def draw_field(key, part):
    first, second = jax.random.split(key, 2)
    chan_scale = jnp.exp(jax.random.uniform(second, (C, 1, 1, 1), jnp.float32, math.log(0.3), math.log(3.0)))
    along_x = jnp.arange(NX, dtype=jnp.float32) / (NX - 1)
    along_y = jnp.arange(NY, dtype=jnp.float32) / (NY - 1)
    ramp = jnp.exp(math.log(3.0) * (along_x[:, None, None] + along_y[None, :, None]) - math.log(3.0))
    base = jnp.clip(jax.random.normal(first, (C, NX, NY, NZ), jnp.float32), -4.0, 4.0)
    return base * chan_scale * ramp[None]


def noise(own_key, shape, spread, reach, kind=jnp.bfloat16):
    drawn = jax.random.normal(own_key, shape, jnp.float32) * spread
    return jnp.minimum(jnp.maximum(drawn, -reach), reach).astype(kind)


def setup_inputs(seed: int = 0, part: int = 0) -> dict:
    splits = jax.random.split(jax.random.key(seed), 12)
    part_splits = jax.random.split(jax.random.fold_in(splits[11], part), 12)
    field = draw_field(jax.random.fold_in(jax.random.fold_in(splits[11], part), 71), part)
    mix_weight = noise(splits[1], (C, C), C ** -0.5, 0.375, jnp.float32)
    factor_x = noise(splits[2], (C, KX), 1.3, 6.0, jnp.float32)
    factor_y = noise(splits[3], (C, KY), 1.3, 6.0, jnp.float32)
    factor_z = noise(splits[4], (C, KZ), 1.3, 6.0, jnp.float32)
    norm_gain = jnp.clip(jax.random.uniform(splits[5], (C,), jnp.float32, 0.5, 1.5), 0.5, 1.5)
    norm_bias = noise(splits[6], (C,), 0.5, 3.0, jnp.float32)
    w_in = noise(splits[7], (HID, C), C ** -0.5, 0.375, jnp.float32)
    b_in = noise(splits[8], (HID,), 0.5, 3.0, jnp.float32)
    w_out = noise(splits[9], (C, HID), HID ** -0.5, 0.375, jnp.float32)
    b_out = noise(splits[10], (C,), 0.5, 3.0, jnp.float32)
    return dict(field=field, mix_weight=mix_weight, factor_x=factor_x, factor_y=factor_y, factor_z=factor_z, norm_gain=norm_gain, norm_bias=norm_bias, w_in=w_in, b_in=b_in, w_out=w_out, b_out=b_out)


def contract(formula, left, right):
    return jnp.einsum(formula, left, right, precision=lax.Precision.HIGHEST)

def tables(length, kept_count):
    indices = jnp.arange(kept_count, dtype=jnp.int32)
    kept_freq = jnp.where(indices < kept_count // 2, indices, length - kept_count + indices)
    positions = jnp.arange(length, dtype=jnp.int32)
    phases = kept_freq[:, None] * positions[None, :] % length
    angles = 2.0 * math.pi / length * phases.astype(jnp.float32)
    return (jnp.cos(angles), jnp.sin(angles))

def transform(planes, cosine, sine, formula):
    real_part = contract(formula, planes[0], cosine) + contract(formula, planes[1], sine)
    imag_part = contract(formula, planes[1], cosine) - contract(formula, planes[0], sine)
    return jnp.stack([real_part, imag_part])

def reference(field, mix_weight, factor_x, factor_y, factor_z, norm_gain, norm_bias, w_in, b_in, w_out, b_out):
    cos_x, sin_x = tables(NX, KX)
    cos_y, sin_y = tables(NY, KY)
    cos_z, sin_z = tables(NZ, KZ)
    planes = jnp.stack([contract('cxyz,kz->cxyk', field, cos_z / NZ), -contract('cxyz,kz->cxyk', field, sin_z / NZ)])
    planes = transform(planes, cos_y / NY, sin_y / NY, 'cxyk,jy->cxjk')
    spectra = transform(planes, cos_x / NX, sin_x / NX, 'cxjk,ix->cijk')
    weighting = factor_x[:, :, None, None] * factor_y[:, None, :, None] * factor_z[:, None, None, :]
    mixed_modes = jnp.einsum('oc,rcijk->roijk', mix_weight, spectra * weighting[None], precision=lax.Precision.HIGHEST)
    returned = transform(mixed_modes, cos_x, -sin_x, 'cijk,ix->cxjk')
    returned = transform(returned, cos_y, -sin_y, 'cxjk,jy->cxyk')
    spectral = contract('cxyk,kz->cxyz', returned[0], cos_z) - contract('cxyk,kz->cxyz', returned[1], sin_z)
    summed = field + spectral
    cells_group = C // GROUPS * NX * NY * NZ
    grouped = summed.reshape(GROUPS, -1)
    group_mean = lax.optimization_barrier(jnp.sum(grouped, axis=1)) / cells_group
    centered = grouped - group_mean[:, None]
    group_var = lax.optimization_barrier(jnp.sum(centered * centered, axis=1)) / cells_group
    inv_scale = jnp.repeat(lax.rsqrt(group_var + 1e-05), C // GROUPS) * norm_gain
    mean_chan = jnp.repeat(group_mean, C // GROUPS)
    columns = summed.reshape(C, -1)
    normed = (columns - mean_chan[:, None]) * inv_scale[:, None] + norm_bias[:, None]
    hidden = jax.nn.gelu(jnp.dot(w_in, normed, precision=lax.Precision.HIGHEST) + b_in[:, None])
    result = columns + jnp.dot(w_out, hidden, precision=lax.Precision.HIGHEST) + b_out[:, None]
    return result.reshape(C, NX, NY, NZ)
```

```python
import math
import functools

import jax
import jax.numpy as jnp
from jax import lax
from jax.experimental import pallas as pl
from jax.experimental.pallas import tpu as pltpu
from jax.sharding import PartitionSpec as P

GROUPS = 32
HIGH = lax.Precision.HIGH
WIDE = ("sp", "rep")


def trig(length, freq, positions):
    phases = (freq[:, None] * positions[None, :]) % length
    angles = 2.0 * math.pi / length * phases.astype(jnp.float32)
    return jnp.cos(angles), jnp.sin(angles)


def kron_pair(cos_a, sin_a, cos_b, sin_b):
    ca, sa = cos_a.T[:, None, :, None], sin_a.T[:, None, :, None]
    cb, sb = cos_b.T[None, :, None, :], sin_b.T[None, :, None, :]
    return ca * cb - sa * sb, sa * cb + ca * sb


def split(value):
    high = value.astype(jnp.bfloat16)
    low = (value - high.astype(jnp.float32)).astype(jnp.bfloat16)
    return high, low


def dot3(left, right):
    lh, ll = left
    rh, rl = right
    d = functools.partial(jnp.dot, preferred_element_type=jnp.float32)
    return d(lh, rh) + (d(lh, rl) + d(ll, rh))


def sum_kernel(field_ref, modes_ref, table_ref, summed_ref, first_ref, second_ref, acc1, acc2):
    step = pl.program_id(0)
    chans, cells, width = field_ref.shape
    rank = modes_ref.shape[2]

    @pl.when(step == 0)
    def _():
        acc1[...] = jnp.zeros_like(acc1)
        acc2[...] = jnp.zeros_like(acc2)

    table = split(table_ref[...])
    chunk = 32 if chans % 32 == 0 else chans

    def body(index, carry):
        rows = pl.ds(pl.multiple_of(index * chunk, chunk), chunk)
        modes = modes_ref[rows].reshape(chunk * cells, rank)
        value = dot3(split(modes), table).reshape(chunk, cells, width) + field_ref[rows]
        summed_ref[rows] = value
        acc1[rows] += value
        acc2[rows] += value * value
        return carry

    lax.fori_loop(0, chans // chunk, body, 0)

    @pl.when(step == pl.num_programs(0) - 1)
    def _():
        first_ref[...] = jnp.sum(acc1[...], axis=1)
        second_ref[...] = jnp.sum(acc2[...], axis=1)


def mlp_kernel(summed_ref, vec_ref, w_in_ref, w_out_ref, out_ref):
    cells = summed_ref.shape[1]
    w_in = split(w_in_ref[...])
    w_out = split(w_out_ref[...])
    vec = vec_ref[...]
    mean, scale, bias = vec[:, 0:1], vec[:, 1:2], vec[:, 2:3]
    b_in, b_out = vec[:, 3:4], vec[:, 4:5]
    pair = 2 if cells % 2 == 0 else 1
    for start in range(0, cells, pair):
        parts = [summed_ref[:, p, :] for p in range(start, start + pair)]
        value = jnp.concatenate(parts, axis=1) if pair > 1 else parts[0]
        normed = (value - mean) * scale + bias
        hidden = dot3(w_in, split(normed)) + b_in
        inner = math.sqrt(2.0 / math.pi) * (hidden + 0.044715 * (hidden * hidden * hidden))
        hidden = hidden * (0.5 * (1.0 + jnp.tanh(inner)))
        result = value + dot3(w_out, split(hidden)) + b_out
        width = summed_ref.shape[2]
        for k in range(pair):
            out_ref[:, start + k, :] = result[:, k * width : (k + 1) * width]


def local(
    field, mix_weight, factor_x, factor_y, factor_z, norm_gain, norm_bias, w_in, b_in, w_out, b_out
):
    wide_count = lax.axis_size(WIDE)
    narrow_count = lax.axis_size("sub")
    own_chans, x_local, ny, nz = field.shape
    chans = own_chans * wide_count
    nx = x_local * narrow_count
    kx, ky, kz = factor_x.shape[1], factor_y.shape[1], factor_z.shape[1]
    y_local = ny // wide_count
    half = kz // 2
    kept = half + 1
    me_sub = lax.axis_index("sub")
    cells = x_local * y_local

    spatial = lax.all_to_all(field, WIDE, split_axis=2, concat_axis=0, tiled=True)

    cos_z, sin_z = trig(nz, jnp.arange(kept), jnp.arange(nz))
    forward = jnp.concatenate([cos_z, -sin_z]) / nz
    planes = jnp.einsum("rz,cxyz->rcxy", forward, field, precision=HIGH)
    planes = planes.reshape(2 * kept * own_chans, x_local * ny)

    def freqs(length, count):
        index = jnp.arange(count)
        return jnp.where(index < count // 2, index, length - count + index)

    cos_y, sin_y = trig(ny, freqs(ny, ky), jnp.arange(ny))

    def forward_xy(values, owner):
        cos_x, sin_x = trig(nx, freqs(nx, kx), owner * x_local + jnp.arange(x_local))
        c, s = kron_pair(cos_x, sin_x, cos_y, sin_y)
        c = (c / (nx * ny)).reshape(x_local * ny, kx * ky)
        s = (s / (nx * ny)).reshape(x_local * ny, kx * ky)
        a = jnp.dot(values, jnp.concatenate([c, s], axis=1), precision=HIGH)
        a = a.reshape(2, kept * own_chans, 2, kx * ky)
        return a[0, :, 0] + a[1, :, 1], a[1, :, 0] - a[0, :, 1]

    held = planes
    real, imag = forward_xy(held, me_sub)
    for hop in range(1, narrow_count):
        held = lax.ppermute(held, "sub", [(i, (i + 1) % narrow_count) for i in range(narrow_count)])
        owner = (me_sub - hop + narrow_count) % narrow_count
        more_real, more_imag = forward_xy(held, owner)
        real, imag = real + more_real, imag + more_imag

    start = lax.axis_index(WIDE) * own_chans
    fx = lax.dynamic_slice_in_dim(factor_x, start, own_chans, 0)
    fy = lax.dynamic_slice_in_dim(factor_y, start, own_chans, 0)
    fz = lax.dynamic_slice_in_dim(factor_z, start, own_chans, 0)
    mirror_x = (-jnp.arange(kx)) % kx
    mirror_y = (-jnp.arange(ky)) % ky
    plane_a = (fx[:, :, None] * fy[:, None, :]).reshape(own_chans, kx * ky)
    plane_b = (fx[:, mirror_x][:, :, None] * fy[:, mirror_y][:, None, :]).reshape(own_chans, kx * ky)
    zero = jnp.zeros((own_chans, 1), jnp.float32)
    z_plus = jnp.concatenate([fz[:, :half], zero], axis=1).T
    z_minus = jnp.concatenate([zero, fz[:, half:][:, ::-1]], axis=1).T
    weight = z_plus[:, :, None] * plane_a[None] + z_minus[:, :, None] * plane_b[None]
    weight = weight.reshape(kept * own_chans, kx * ky)
    real, imag = real * weight, imag * weight

    cos_x, sin_x = trig(nx, freqs(nx, kx), me_sub * x_local + jnp.arange(x_local))
    c, s = kron_pair(cos_x, sin_x, cos_y, sin_y)

    def columns(t):
        t = t.reshape(x_local, wide_count, y_local, kx * ky)
        return t.transpose(3, 1, 0, 2).reshape(kx * ky, wide_count * cells)

    c, s = columns(c), columns(s)
    table_re = jnp.concatenate([c, -s])
    table_im = jnp.concatenate([s, c])
    both = jnp.concatenate([real, imag], axis=1)
    back = jnp.stack(
        [jnp.dot(both, table_re, precision=HIGH), jnp.dot(both, table_im, precision=HIGH)]
    )
    back = back.reshape(2 * kept, own_chans, wide_count, cells)
    back = back.transpose(2, 1, 0, 3).reshape(wide_count * own_chans, 2 * kept * cells)
    back = lax.all_to_all(back, WIDE, split_axis=0, concat_axis=0, tiled=True)
    back = back.reshape(chans, 2 * kept, cells)
    mixed = jnp.einsum("oi,irp->opr", mix_weight, back, precision=HIGH)

    inverse_z = jnp.concatenate([cos_z, -sin_z])
    spatial = spatial.reshape(chans, cells, nz)
    block = 8 if cells % 8 == 0 else cells
    steps = cells // block
    cube = pl.BlockSpec((chans, block, nz), lambda i: (0, i, 0))
    whole = lambda *shape: pl.BlockSpec(shape, lambda i: (0,) * len(shape))
    summed, first, second = pl.pallas_call(
        sum_kernel,
        grid=(steps,),
        out_shape=(
            jax.ShapeDtypeStruct(spatial.shape, jnp.float32),
            jax.ShapeDtypeStruct((chans, nz), jnp.float32),
            jax.ShapeDtypeStruct((chans, nz), jnp.float32),
        ),
        in_specs=[
            cube,
            pl.BlockSpec((chans, block, 2 * kept), lambda i: (0, i, 0)),
            whole(2 * kept, nz),
        ],
        out_specs=(cube, whole(chans, nz), whole(chans, nz)),
        scratch_shapes=[pltpu.VMEM((chans, block, nz), jnp.float32)] * 2,
        name="sum_stats",
    )(spatial, mixed, inverse_z)

    size = chans // GROUPS
    stats = jnp.stack([first, second]).reshape(2, GROUPS, size * nz).sum(axis=2)
    everyone = ("sp", "sub", "rep")
    stats = lax.all_gather(stats, everyone).reshape(-1, 2, GROUPS).sum(axis=0)
    cells_group = size * nx * ny * nz
    group_mean = stats[0] / cells_group
    group_var = stats[1] / cells_group - group_mean * group_mean
    scale = jnp.repeat(lax.rsqrt(group_var + 1e-05), size) * norm_gain
    mean = jnp.repeat(group_mean, size)
    vec = jnp.stack([mean, scale, norm_bias, b_in, b_out] + [b_out] * 3, axis=1)

    result = pl.pallas_call(
        mlp_kernel,
        grid=(steps,),
        out_shape=jax.ShapeDtypeStruct(spatial.shape, jnp.float32),
        in_specs=[cube, whole(chans, 8), whole(*w_in.shape), whole(*w_out.shape)],
        out_specs=cube,
        name="mlp",
    )(summed, vec, w_in, w_out)
    return result.reshape(chans, x_local, y_local, nz)


def solution(mesh):
    placed = (P(("grp", "sp", "rep"), "sub", None, None),) + (P(),) * 10
    return jax.shard_map(
        local,
        mesh=mesh,
        in_specs=placed,
        out_specs=P("grp", "sub", ("sp", "rep"), None),
        check_vma=False,
    )
```

```python
import math
import functools

import jax
import jax.numpy as jnp
from jax import lax
from jax.experimental import pallas as pl
from jax.experimental.pallas import tpu as pltpu
from jax.sharding import PartitionSpec as P

GROUPS = 32
HIGH = lax.Precision.HIGH
WIDE = ("sp", "rep")


def trig(length, freq, positions):
    phases = (freq[:, None] * positions[None, :]) % length
    angles = 2.0 * math.pi / length * phases.astype(jnp.float32)
    return jnp.cos(angles), jnp.sin(angles)


def kron_pair(cos_a, sin_a, cos_b, sin_b):
    ca, sa = cos_a.T[:, None, :, None], sin_a.T[:, None, :, None]
    cb, sb = cos_b.T[None, :, None, :], sin_b.T[None, :, None, :]
    return ca * cb - sa * sb, sa * cb + ca * sb


def split(value):
    high = value.astype(jnp.bfloat16)
    low = (value - high.astype(jnp.float32)).astype(jnp.bfloat16)
    return high, low


def dot3(left, right):
    lh, ll = left
    rh, rl = right
    d = functools.partial(jnp.dot, preferred_element_type=jnp.float32)
    return d(lh, rh) + (d(lh, rl) + d(ll, rh))


def sum_kernel(field_ref, modes_ref, table_ref, summed_ref, first_ref, second_ref, acc1, acc2):
    step = pl.program_id(0)
    chans, cells, width = field_ref.shape
    rank = modes_ref.shape[2]

    @pl.when(step == 0)
    def _():
        acc1[...] = jnp.zeros_like(acc1)
        acc2[...] = jnp.zeros_like(acc2)

    table = split(table_ref[...])
    chunk = 32 if chans % 32 == 0 else chans

    def body(index, carry):
        rows = pl.ds(pl.multiple_of(index * chunk, chunk), chunk)
        modes = modes_ref[rows].reshape(chunk * cells, rank)
        value = dot3(split(modes), table).reshape(chunk, cells, width) + field_ref[rows]
        summed_ref[rows] = value
        acc1[rows] += value
        acc2[rows] += value * value
        return carry

    lax.fori_loop(0, chans // chunk, body, 0)

    @pl.when(step == pl.num_programs(0) - 1)
    def _():
        first_ref[...] = jnp.sum(acc1[...], axis=1)
        second_ref[...] = jnp.sum(acc2[...], axis=1)


def mlp_kernel(summed_ref, vec_ref, w_in_ref, w_out_ref, out_ref):
    cells = summed_ref.shape[1]
    w_in = split(w_in_ref[...])
    w_out = split(w_out_ref[...])
    vec = vec_ref[...]
    mean, scale, bias = vec[:, 0:1], vec[:, 1:2], vec[:, 2:3]
    b_in, b_out = vec[:, 3:4], vec[:, 4:5]
    pair = 2 if cells % 2 == 0 else 1
    for start in range(0, cells, pair):
        parts = [summed_ref[:, p, :] for p in range(start, start + pair)]
        value = jnp.concatenate(parts, axis=1) if pair > 1 else parts[0]
        normed = (value - mean) * scale + bias
        hidden = dot3(w_in, split(normed)) + b_in
        inner = math.sqrt(2.0 / math.pi) * (hidden + 0.044715 * (hidden * hidden * hidden))
        hidden = hidden * (0.5 * (1.0 + jnp.tanh(inner)))
        result = value + dot3(w_out, split(hidden)) + b_out
        width = summed_ref.shape[2]
        for k in range(pair):
            out_ref[:, start + k, :] = result[:, k * width : (k + 1) * width]


def local(
    field, mix_weight, factor_x, factor_y, factor_z, norm_gain, norm_bias, w_in, b_in, w_out, b_out
):
    wide_count = lax.axis_size(WIDE)
    narrow_count = lax.axis_size("sub")
    own_chans, x_local, ny, nz = field.shape
    chans = own_chans * wide_count
    nx = x_local * narrow_count
    kx, ky, kz = factor_x.shape[1], factor_y.shape[1], factor_z.shape[1]
    y_local = ny // wide_count
    half = kz // 2
    kept = half + 1
    me_sub = lax.axis_index("sub")
    cells = x_local * y_local

    spatial = lax.all_to_all(field, WIDE, split_axis=2, concat_axis=0, tiled=True)

    cos_z, sin_z = trig(nz, jnp.arange(kept), jnp.arange(nz))
    forward = jnp.concatenate([cos_z, -sin_z]) / nz
    planes = jnp.einsum("rz,cxyz->rcxy", forward, field, precision=HIGH)
    planes = planes.reshape(2 * kept * own_chans, x_local * ny)

    def freqs(length, count):
        index = jnp.arange(count)
        return jnp.where(index < count // 2, index, length - count + index)

    cos_y, sin_y = trig(ny, freqs(ny, ky), jnp.arange(ny))

    def forward_xy(values, owner):
        cos_x, sin_x = trig(nx, freqs(nx, kx), owner * x_local + jnp.arange(x_local))
        c, s = kron_pair(cos_x, sin_x, cos_y, sin_y)
        c = (c / (nx * ny)).reshape(x_local * ny, kx * ky)
        s = (s / (nx * ny)).reshape(x_local * ny, kx * ky)
        a = jnp.dot(values, jnp.concatenate([c, s], axis=1), precision=HIGH)
        a = a.reshape(2, kept * own_chans, 2, kx * ky)
        return a[0, :, 0] + a[1, :, 1], a[1, :, 0] - a[0, :, 1]

    held = planes
    real, imag = forward_xy(held, me_sub)
    for hop in range(1, narrow_count):
        held = lax.ppermute(held, "sub", [(i, (i + 1) % narrow_count) for i in range(narrow_count)])
        owner = (me_sub - hop + narrow_count) % narrow_count
        more_real, more_imag = forward_xy(held, owner)
        real, imag = real + more_real, imag + more_imag

    start = lax.axis_index(WIDE) * own_chans
    fx = lax.dynamic_slice_in_dim(factor_x, start, own_chans, 0)
    fy = lax.dynamic_slice_in_dim(factor_y, start, own_chans, 0)
    fz = lax.dynamic_slice_in_dim(factor_z, start, own_chans, 0)
    mirror_x = (-jnp.arange(kx)) % kx
    mirror_y = (-jnp.arange(ky)) % ky
    plane_a = (fx[:, :, None] * fy[:, None, :]).reshape(own_chans, kx * ky)
    plane_b = (fx[:, mirror_x][:, :, None] * fy[:, mirror_y][:, None, :]).reshape(own_chans, kx * ky)
    zero = jnp.zeros((own_chans, 1), jnp.float32)
    z_plus = jnp.concatenate([fz[:, :half], zero], axis=1).T
    z_minus = jnp.concatenate([zero, fz[:, half:][:, ::-1]], axis=1).T
    weight = z_plus[:, :, None] * plane_a[None] + z_minus[:, :, None] * plane_b[None]
    weight = weight.reshape(kept * own_chans, kx * ky)
    real, imag = real * weight, imag * weight

    cos_x, sin_x = trig(nx, freqs(nx, kx), me_sub * x_local + jnp.arange(x_local))
    c, s = kron_pair(cos_x, sin_x, cos_y, sin_y)

    def columns(t):
        t = t.reshape(x_local, wide_count, y_local, kx * ky)
        return t.transpose(3, 1, 0, 2).reshape(kx * ky, wide_count * cells)

    c, s = columns(c), columns(s)
    table_re = jnp.concatenate([c, -s])
    table_im = jnp.concatenate([s, c])
    both = jnp.concatenate([real, imag], axis=1)
    back = jnp.stack(
        [jnp.dot(both, table_re, precision=HIGH), jnp.dot(both, table_im, precision=HIGH)]
    )
    back = back.reshape(2 * kept, own_chans, wide_count, cells)
    back = back.transpose(2, 1, 0, 3).reshape(wide_count * own_chans, 2 * kept * cells)
    back, spatial = lax.optimization_barrier((back, spatial))
    back = lax.all_to_all(back, WIDE, split_axis=0, concat_axis=0, tiled=True)
    back = back.reshape(chans, 2 * kept, cells)
    mixed = jnp.einsum("oi,irp->opr", mix_weight, back, precision=HIGH)

    inverse_z = jnp.concatenate([cos_z, -sin_z])
    spatial = spatial.reshape(chans, cells, nz)
    block = 8 if cells % 8 == 0 else cells
    steps = cells // block
    cube = pl.BlockSpec((chans, block, nz), lambda i: (0, i, 0))
    whole = lambda *shape: pl.BlockSpec(shape, lambda i: (0,) * len(shape))
    summed, first, second = pl.pallas_call(
        sum_kernel,
        grid=(steps,),
        out_shape=(
            jax.ShapeDtypeStruct(spatial.shape, jnp.float32),
            jax.ShapeDtypeStruct((chans, nz), jnp.float32),
            jax.ShapeDtypeStruct((chans, nz), jnp.float32),
        ),
        in_specs=[
            cube,
            pl.BlockSpec((chans, block, 2 * kept), lambda i: (0, i, 0)),
            whole(2 * kept, nz),
        ],
        out_specs=(cube, whole(chans, nz), whole(chans, nz)),
        scratch_shapes=[pltpu.VMEM((chans, block, nz), jnp.float32)] * 2,
        name="sum_stats",
    )(spatial, mixed, inverse_z)

    size = chans // GROUPS
    stats = jnp.stack([first, second]).reshape(2, GROUPS, size * nz).sum(axis=2)
    everyone = ("sp", "sub", "rep")
    stats = lax.all_gather(stats, everyone).reshape(-1, 2, GROUPS).sum(axis=0)
    cells_group = size * nx * ny * nz
    group_mean = stats[0] / cells_group
    group_var = stats[1] / cells_group - group_mean * group_mean
    scale = jnp.repeat(lax.rsqrt(group_var + 1e-05), size) * norm_gain
    mean = jnp.repeat(group_mean, size)
    vec = jnp.stack([mean, scale, norm_bias, b_in, b_out] + [b_out] * 3, axis=1)

    result = pl.pallas_call(
        mlp_kernel,
        grid=(steps,),
        out_shape=jax.ShapeDtypeStruct(spatial.shape, jnp.float32),
        in_specs=[cube, whole(chans, 8), whole(*w_in.shape), whole(*w_out.shape)],
        out_specs=cube,
        name="mlp",
    )(summed, vec, w_in, w_out)
    return result.reshape(chans, x_local, y_local, nz)


def solution(mesh):
    placed = (P(("grp", "sp", "rep"), "sub", None, None),) + (P(),) * 10
    return jax.shard_map(
        local,
        mesh=mesh,
        in_specs=placed,
        out_specs=P("grp", "sub", ("sp", "rep"), None),
        check_vma=False,
    )
```
